128 devices in a mesh: kx: 8 (over z_lo, y), ky: 16 (over x, z_hi, core).
Axes of the slice: x: 4, y: 4, z: 4 (z_hi: 2, z_lo: 2; z = z_hi * 2 + z_lo), core: 2. Of those that a mesh axis runs over, the one named last changes fastest.
Arguments:
- wannier: bfloat16 [32, 128, 64, 128], P('kx', 'ky'), may hold values from -0.5 to 0.5
- coupling: bfloat16 [3, 32, 128, 6, 64, 128], P(None, 'kx', 'ky'), may hold values from -6 to 6
- kq_map: int32 [3, 4096], replicated, may hold values from 0 to 4095, as said below
Outputs:
- rotated: bfloat16 [3, 32, 128, 6, 64, 128], P(None, 'kx', 'ky')
The draws below stay inside these ranges and needn't reach their ends.
Inputs may be any that keep to these rules, and one draw needn't show every extreme that they name: For every q there are offsets a and b with kq_map[q, x * 128 + y] = ((x + a) mod 32) * 128 + (y + b) mod 128.
All inputs are finite; a program needn't handle non-finite values.
Results may differ from the reference program's by a relative error of at most 0.0049.
Values may be sent and summed in bfloat16 or wider, within the bound.
No kernel may reach another device: no remote copies, remote signals or barrier semaphores. Data moves between devices by JAX's collectives and lax.ppermute only.
A program may use at most 192 MiB of HBM per device.

```python
import jax
import jax.numpy as jnp

NB = 64
MODES = 6
Q = 3
KX_DEV = 4
KY_DEV = 8
NX = 32
NY = 128


def draw_kq_map(key, part):
    blocks_x = jax.random.randint(jax.random.fold_in(key, 11), (Q,), 0, NX // KX_DEV)
    blocks_x = blocks_x.at[0].set(NX // KX_DEV - 1)
    blocks_x = blocks_x.at[1].set(NX // KX_DEV // 2)
    blocks_y = jax.random.randint(jax.random.fold_in(key, 23), (Q,), 0, NY // KY_DEV)
    blocks_y = blocks_y.at[0].set(NY // KY_DEV - 1)
    blocks_y = blocks_y.at[1].set(NY // KY_DEV // 2)
    inner_x = jax.random.randint(jax.random.fold_in(key, 37), (Q,), 1, KX_DEV)
    inner_y = jax.random.randint(jax.random.fold_in(key, 41), (Q,), 1, KY_DEV)
    shift_x = blocks_x * KX_DEV + inner_x
    shift_y = blocks_y * KY_DEV + inner_y
    grid_x = jnp.arange(NX, dtype=jnp.int32)[None, :, None]
    grid_y = jnp.arange(NY, dtype=jnp.int32)[None, None, :]
    mapped = (grid_x + shift_x[:, None, None]) % NX * NY + (grid_y + shift_y[:, None, None]) % NY
    return mapped.reshape(Q, NX * NY).astype(jnp.int32)


def levels(own_key, dims, pieces, low, largest):
    def one(position, blocks):
        steps = jax.random.uniform(jax.random.fold_in(jax.random.fold_in(own_key, 6), position), (blocks,), jnp.float32, low / len(pieces), largest / len(pieces))
        return jnp.repeat(jnp.exp(steps), dims[position] // blocks).reshape((-1,) + (1,) * (len(dims) - position - 1))

    gain = one(*pieces[0])
    for cut in pieces[1:]:
        gain = gain * one(*cut)
    return gain


def centred(own_key, shape, spread, bound, cuts=(), kind=jnp.bfloat16):
    drawn = jax.random.normal(own_key, shape, jnp.float32) * spread
    if len(cuts) > 0:
        drawn = levels(own_key, shape, cuts, -0.22, 0.18) * drawn
    return jnp.clip(drawn, min=-bound, max=bound).astype(kind)


def setup_inputs(seed: int = 0) -> dict:
    key_list = jax.random.split(jax.random.key(seed), 4)
    return {
        "wannier": centred(key_list[0], (NX, NY, NB, 2 * NB), (2 * NB) ** -0.5, 0.5, ((0, 8), (1, 16))),
        "coupling": centred(key_list[1], (Q, NX, NY, MODES, NB, 2 * NB), 1.0, 6.0, ((1, 8), (2, 16))),
        "kq_map": draw_kq_map(jax.random.fold_in(key_list[3], 71), 0),
    }


def right_factor(matrix):
    half_width = matrix.shape[-1] // 2
    lower_half = jnp.concatenate([-matrix[..., half_width:], matrix[..., :half_width]], axis=-1)
    return jnp.concatenate([matrix, lower_half], axis=-2)


def rotate(block_g, factor, partner):
    half_width = partner.shape[-1] // 2
    half_turn = jnp.einsum("xymac,xycd->xymad", block_g.astype(jnp.float32), factor.astype(jnp.float32)).astype(jnp.bfloat16)
    stacked = jnp.concatenate([half_turn, jnp.concatenate([half_turn[..., half_width:], -half_turn[..., :half_width]], axis=-1)], axis=-2)
    partner_rows = jnp.concatenate([partner[..., :half_width], partner[..., half_width:]], axis=-2)
    return jnp.einsum("xyca,xymcd->xymad", partner_rows.astype(jnp.float32), stacked.astype(jnp.float32)).astype(jnp.bfloat16)


def reference(wannier, coupling, kq_map):
    factor = right_factor(wannier)
    flattened = wannier.reshape(NX * NY, NB, 2 * NB)
    results = []
    for qpoint in range(Q):
        partner = flattened[kq_map[qpoint]].reshape(NX, NY, NB, 2 * NB)
        results.append(rotate(coupling[qpoint], factor, partner))
    return jnp.stack(results, axis=0)
```

```python
import jax
import jax.numpy as jnp
from jax import lax
from jax.experimental import pallas as pl
from jax.experimental.pallas import tpu as pltpu
from jax.sharding import PartitionSpec as P

AXES = ("kx", "ky")
MIB = 1024 * 1024
H_GROUPS = 8
R_GROUPS = 16


def stream(in_ref, out_ref, in_buf, out_buf, in_sem, out_sem, work):
    groups = in_sem.shape[0]
    size = in_buf.shape[1] // groups

    def fetch(i):
        at = pl.ds(i * size, size)
        return pltpu.make_async_copy(in_ref.at[:, at], in_buf.at[:, at], in_sem.at[i])

    def send(i):
        at = pl.ds(i * size, size)
        return pltpu.make_async_copy(out_buf.at[:, at], out_ref.at[:, at], out_sem.at[i])

    def start(i, carry):
        fetch(i).start()
        return carry

    def step(i, carry):
        fetch(i).wait()
        for k in range(size):
            work(i * size + k)
        send(i).start()
        return carry

    def finish(i, carry):
        send(i).wait()
        return carry

    lax.fori_loop(0, groups, start, 0)
    lax.fori_loop(0, groups, step, 0)
    lax.fori_loop(0, groups, finish, 0)


def stream_scratch(shape_in, shape_out, groups):
    return [
        pltpu.VMEM(shape_in, jnp.bfloat16),
        pltpu.VMEM(shape_out, jnp.bfloat16),
        pltpu.SemaphoreType.DMA((groups,)),
        pltpu.SemaphoreType.DMA((groups,)),
    ]


def half_turn_kernel(u_ref, g_ref, o_ref, g_buf, o_buf, in_sem, out_sem):
    n_q, _, modes, nb, width = g_buf.shape

    def work(k):
        u = u_ref[k]
        turned = jnp.concatenate([-u[:, nb:], u[:, :nb]], axis=1)
        factor = jnp.concatenate([u, turned], axis=0)
        for q in range(n_q):
            rows = g_buf[q, k].reshape(modes * nb, width)
            half = jnp.dot(rows, factor, preferred_element_type=jnp.float32).astype(jnp.bfloat16)
            for p in range(modes // 2):
                one = half[2 * p * nb : (2 * p + 1) * nb]
                two = half[(2 * p + 1) * nb : (2 * p + 2) * nb]
                o_buf[q, k, p, :nb] = jnp.concatenate([one[:, :nb], two[:, :nb]], axis=1)
                o_buf[q, k, p, nb:] = jnp.concatenate([one[:, nb:], two[:, nb:]], axis=1)

    stream(g_ref, o_ref, g_buf, o_buf, in_sem, out_sem, work)


def half_turns(wannier, coupling):
    n_q, n_k, modes, nb, width = coupling.shape
    paired = (n_q, n_k, modes // 2, 2 * nb, width)
    return pl.pallas_call(
        half_turn_kernel,
        in_specs=[pl.BlockSpec(memory_space=pltpu.VMEM), pl.BlockSpec(memory_space=pltpu.HBM)],
        out_specs=pl.BlockSpec(memory_space=pltpu.HBM),
        out_shape=jax.ShapeDtypeStruct(paired, jnp.bfloat16),
        scratch_shapes=stream_scratch(coupling.shape, paired, H_GROUPS),
        compiler_params=pltpu.CompilerParams(vmem_limit_bytes=56 * MIB),
        cost_estimate=pl.CostEstimate(
            flops=4 * n_q * n_k * modes * nb * width * width,
            bytes_accessed=4 * n_q * n_k * modes * nb * width,
            transcendentals=0,
        ),
        name="half_turns",
    )(wannier, coupling)


def shuffle_kernel(shift_ref, held_ref, o_ref):
    n_x, n_y, rows, _ = held_ref.shape
    for q in range(o_ref.shape[2] // rows):
        shift_x = shift_ref[q, 0]
        shift_y = shift_ref[q, 1]
        for y in range(n_y):
            from_y = lax.rem(shift_y + y, n_y)
            for x in range(n_x):
                o_ref[x, y, q * rows : (q + 1) * rows] = held_ref[lax.rem(shift_x + x, n_x), from_y]


def shuffle(shifts, held, n_q):
    n_x, n_y, rows, width = held.shape
    return pl.pallas_call(
        shuffle_kernel,
        in_specs=[
            pl.BlockSpec(memory_space=pltpu.SMEM),
            pl.BlockSpec(memory_space=pltpu.VMEM),
        ],
        out_specs=pl.BlockSpec(memory_space=pltpu.VMEM),
        out_shape=jax.ShapeDtypeStruct((n_x, n_y, n_q * rows, width), held.dtype),
        compiler_params=pltpu.CompilerParams(vmem_limit_bytes=8 * MIB),
        name="shuffle",
    )(shifts, held)


def rotate_kernel(shift_ref, v_ref, h_ref, o_ref, h_buf, o_buf, in_sem, out_sem, *, n_x, n_y):
    n_q, _, modes, nb, width = o_buf.shape
    rows = v_ref.shape[2] // n_q

    def work(k):
        for q in range(n_q):
            at_x = lax.rem(k // n_y + shift_ref[q, 2], n_x)
            at_y = lax.rem(lax.rem(k, n_y) + shift_ref[q, 3], n_y)
            v = v_ref[at_x * n_y + at_y, :, q * rows : (q + 1) * rows].reshape(nb, width)
            left = jnp.concatenate(
                [
                    jnp.concatenate([v[:, :nb], -v[:, nb:]], axis=1),
                    jnp.concatenate([v[:, nb:], v[:, :nb]], axis=1),
                ],
                axis=0,
            )
            right = jnp.concatenate([h_buf[q, k, p] for p in range(modes // 2)], axis=1)
            out = lax.dot_general(
                left, right, (((0,), (0,)), ((), ())), preferred_element_type=jnp.float32
            ).astype(jnp.bfloat16)
            for p in range(modes // 2):
                real = out[:nb, p * width : (p + 1) * width]
                imag = out[nb:, p * width : (p + 1) * width]
                o_buf[q, k, 2 * p] = jnp.concatenate([real[:, :nb], imag[:, :nb]], axis=1)
                o_buf[q, k, 2 * p + 1] = jnp.concatenate([real[:, nb:], imag[:, nb:]], axis=1)

    stream(h_ref, o_ref, h_buf, o_buf, in_sem, out_sem, work)


def rotate(shifts, partner, halves, n_x, n_y):
    n_q, n_k, pairs, _, width = halves.shape
    modes, nb = 2 * pairs, width // 2
    shape = (n_q, n_k, modes, nb, width)
    return pl.pallas_call(
        lambda *refs: rotate_kernel(*refs, n_x=n_x, n_y=n_y),
        in_specs=[
            pl.BlockSpec(memory_space=pltpu.SMEM),
            pl.BlockSpec(memory_space=pltpu.VMEM),
            pl.BlockSpec(memory_space=pltpu.HBM),
        ],
        out_specs=pl.BlockSpec(memory_space=pltpu.HBM),
        out_shape=jax.ShapeDtypeStruct(shape, jnp.bfloat16),
        scratch_shapes=stream_scratch(halves.shape, shape, R_GROUPS),
        compiler_params=pltpu.CompilerParams(vmem_limit_bytes=50 * MIB),
        cost_estimate=pl.CostEstimate(
            flops=4 * n_q * n_k * modes * nb * width * nb,
            bytes_accessed=4 * n_q * n_k * modes * nb * width,
            transcendentals=0,
        ),
        name="rotate",
    )(shifts, partner, halves)


def per_device(wannier, coupling, kq_map):
    rows_x, cols_y, nb, width = wannier.shape
    n_q = coupling.shape[0]
    modes = coupling.shape[3]
    count_x = lax.axis_size("kx")
    count_y = lax.axis_size("ky")
    devices = count_x * count_y
    n_k = rows_x * cols_y
    pieces = devices // n_k
    rows = nb // pieces
    total_y = cols_y * count_y
    me = lax.axis_index("kx") * count_y + lax.axis_index("ky")
    point = me // pieces
    offset = kq_map[:, 0]
    offset_x = offset // total_y
    offset_y = offset % total_y
    inner_x = offset_x % rows_x
    inner_y = offset_y % cols_y
    carry_x = (point // cols_y < inner_x).astype(jnp.int32)
    carry_y = (point % cols_y < inner_y).astype(jnp.int32)
    shifts = jnp.stack(
        [offset_x // rows_x + carry_x, offset_y // cols_y + carry_y, inner_x, inner_y], axis=1
    )

    spread = lax.all_to_all(wannier.reshape(devices, rows, width), AXES, 0, 0, tiled=True)
    halves = half_turns(
        wannier.reshape(n_k, nb, width), coupling.reshape(n_q, n_k, modes, nb, width)
    )
    outgoing = shuffle(shifts, spread.reshape(count_x, count_y, rows, width), n_q)
    back = lax.all_to_all(outgoing.reshape(devices, n_q * rows, width), AXES, 0, 0, tiled=True)
    partner = back.reshape(n_k, pieces, n_q * rows, width)
    rotated = rotate(shifts, partner, halves, rows_x, cols_y)
    return rotated.reshape(coupling.shape)


def solution(mesh):
    in_specs = (P("kx", "ky", None, None), P(None, "kx", "ky", None, None, None), P())
    out_specs = P(None, "kx", "ky", None, None, None)
    return jax.shard_map(
        per_device, mesh=mesh, in_specs=in_specs, out_specs=out_specs, check_vma=False
    )
```

```python
import jax
import jax.numpy as jnp
from jax import lax
from jax.experimental import pallas as pl
from jax.experimental.pallas import tpu as pltpu
from jax.sharding import PartitionSpec as P

AXES = ("kx", "ky")
MIB = 1024 * 1024
H_GROUPS = 8
R_GROUPS = 16


def stream(in_ref, out_ref, in_buf, out_buf, in_sem, out_sem, work):
    groups = in_sem.shape[0]
    size = in_buf.shape[1] // groups

    def fetch(i):
        at = pl.ds(i * size, size)
        return pltpu.make_async_copy(in_ref.at[:, at], in_buf.at[:, at], in_sem.at[i])

    def send(i):
        at = pl.ds(i * size, size)
        return pltpu.make_async_copy(out_buf.at[:, at], out_ref.at[:, at], out_sem.at[i])

    def start(i, carry):
        fetch(i).start()
        return carry

    def step(i, carry):
        fetch(i).wait()
        for k in range(size):
            work(i * size + k)
        send(i).start()
        return carry

    def finish(i, carry):
        send(i).wait()
        return carry

    lax.fori_loop(0, groups, start, 0)
    lax.fori_loop(0, groups, step, 0)
    lax.fori_loop(0, groups, finish, 0)


def stream_scratch(shape_in, shape_out, groups):
    return [
        pltpu.VMEM(shape_in, jnp.bfloat16),
        pltpu.VMEM(shape_out, jnp.bfloat16),
        pltpu.SemaphoreType.DMA((groups,)),
        pltpu.SemaphoreType.DMA((groups,)),
    ]


def half_turn_kernel(u_ref, g_ref, o_ref, g_buf, o_buf, in_sem, out_sem):
    n_q, _, modes, nb, width = g_buf.shape

    def work(k):
        u = u_ref[k]
        turned = jnp.concatenate([-u[:, nb:], u[:, :nb]], axis=1)
        factor = jnp.concatenate([u, turned], axis=0)
        for q in range(n_q):
            rows = g_buf[q, k].reshape(modes * nb, width)
            half = jnp.dot(rows, factor, preferred_element_type=jnp.float32).astype(jnp.bfloat16)
            for p in range(modes // 2):
                one = half[2 * p * nb : (2 * p + 1) * nb]
                two = half[(2 * p + 1) * nb : (2 * p + 2) * nb]
                o_buf[q, k, :nb, p * width : (p + 1) * width] = jnp.concatenate([one[:, :nb], two[:, :nb]], axis=1)
                o_buf[q, k, nb:, p * width : (p + 1) * width] = jnp.concatenate([one[:, nb:], two[:, nb:]], axis=1)

    stream(g_ref, o_ref, g_buf, o_buf, in_sem, out_sem, work)


def half_turns(wannier, coupling):
    n_q, n_k, modes, nb, width = coupling.shape
    paired = (n_q, n_k, 2 * nb, modes // 2 * width)
    return pl.pallas_call(
        half_turn_kernel,
        in_specs=[pl.BlockSpec(memory_space=pltpu.VMEM), pl.BlockSpec(memory_space=pltpu.HBM)],
        out_specs=pl.BlockSpec(memory_space=pltpu.HBM),
        out_shape=jax.ShapeDtypeStruct(paired, jnp.bfloat16),
        scratch_shapes=stream_scratch(coupling.shape, paired, H_GROUPS),
        compiler_params=pltpu.CompilerParams(vmem_limit_bytes=56 * MIB),
        cost_estimate=pl.CostEstimate(
            flops=4 * n_q * n_k * modes * nb * width * width,
            bytes_accessed=4 * n_q * n_k * modes * nb * width,
            transcendentals=0,
        ),
        name="half_turns",
    )(wannier, coupling)


def shuffle_kernel(shift_ref, held_ref, o_ref):
    n_x, n_y, rows, _ = held_ref.shape
    for q in range(o_ref.shape[2] // rows):
        shift_x = shift_ref[q, 0]
        shift_y = shift_ref[q, 1]
        for y in range(n_y):
            from_y = lax.rem(shift_y + y, n_y)
            for x in range(n_x):
                o_ref[x, y, q * rows : (q + 1) * rows] = held_ref[lax.rem(shift_x + x, n_x), from_y]


def shuffle(shifts, held, n_q):
    n_x, n_y, rows, width = held.shape
    return pl.pallas_call(
        shuffle_kernel,
        in_specs=[
            pl.BlockSpec(memory_space=pltpu.SMEM),
            pl.BlockSpec(memory_space=pltpu.VMEM),
        ],
        out_specs=pl.BlockSpec(memory_space=pltpu.VMEM),
        out_shape=jax.ShapeDtypeStruct((n_x, n_y, n_q * rows, width), held.dtype),
        compiler_params=pltpu.CompilerParams(vmem_limit_bytes=8 * MIB),
        name="shuffle",
    )(shifts, held)


def rotate_kernel(
    shift_ref, v_ref, h_ref, o_ref, h_buf, o_buf, in_sem, out_sem, left_a, left_b, raw_a, raw_b, *, n_x, n_y
):
    n_q, n_k, modes, nb, width = o_buf.shape
    rows = v_ref.shape[2] // n_q
    pairs = modes // 2
    groups = in_sem.shape[0]
    size = n_k // groups
    units = [(q, k) for k in range(size) for q in range(n_q)]

    def fetch(i):
        at = pl.ds(i * size, size)
        return pltpu.make_async_copy(h_ref.at[:, at], h_buf.at[:, at], in_sem.at[i])

    def send(i):
        at = pl.ds(i * size, size)
        return pltpu.make_async_copy(o_buf.at[:, at], o_ref.at[:, at], out_sem.at[i])

    def prepare(i, left_ref):
        for u, (q, k) in enumerate(units):
            at = i * size + k
            at_x = lax.rem(at // n_y + shift_ref[q, 2], n_x)
            at_y = lax.rem(lax.rem(at, n_y) + shift_ref[q, 3], n_y)
            v = v_ref[at_x * n_y + at_y, :, q * rows : (q + 1) * rows].reshape(nb, width)
            left = jnp.concatenate(
                [
                    jnp.concatenate([v[:, :nb], -v[:, nb:]], axis=1),
                    jnp.concatenate([v[:, nb:], v[:, :nb]], axis=1),
                ],
                axis=0,
            )
            left_ref[u] = left.T

    def multiply(i, left_ref, raw_ref):
        for u, (q, k) in enumerate(units):
            right = h_buf[q, i * size + k]
            out = jnp.dot(left_ref[u], right, preferred_element_type=jnp.float32)
            raw_ref[u] = out

    lane = lax.broadcasted_iota(jnp.int32, (nb, width), 1)

    def arrange(i, raw_ref):
        for u, (q, k) in enumerate(units):
            at = i * size + k
            for p in range(pairs):
                real = raw_ref[u, :nb, p * width : (p + 1) * width]
                imag = raw_ref[u, nb:, p * width : (p + 1) * width]
                outer = jnp.where(lane < nb, real, imag)
                inner = pltpu.roll(jnp.where(lane < nb, imag, real), nb, 1)
                one = jnp.where(lane < nb, outer, inner)
                two = jnp.where(lane < nb, inner, outer)
                o_buf[q, at, 2 * p] = one.astype(jnp.bfloat16)
                o_buf[q, at, 2 * p + 1] = two.astype(jnp.bfloat16)

    def start(i, carry):
        fetch(i).start()
        return carry

    def step(j, carry):
        i = 2 * j
        last = jnp.maximum(i - 1, 0)
        fetch(i).wait()
        multiply(i, left_a, raw_a)
        prepare(i + 1, left_b)
        arrange(last, raw_b)

        @pl.when(j > 0)
        def _():
            send(last).start()

        fetch(i + 1).wait()
        multiply(i + 1, left_b, raw_b)
        prepare(jnp.minimum(i + 2, groups - 1), left_a)
        arrange(i, raw_a)
        send(i).start()
        return carry

    def finish(i, carry):
        send(i).wait()
        return carry

    lax.fori_loop(0, groups, start, 0)
    prepare(0, left_a)
    lax.fori_loop(0, groups // 2, step, 0)
    arrange(groups - 1, raw_b)
    send(groups - 1).start()
    lax.fori_loop(0, groups, finish, 0)


def rotate(shifts, partner, halves, n_x, n_y):
    n_q, n_k, width, columns = halves.shape
    pairs, nb = columns // width, width // 2
    modes = 2 * pairs
    shape = (n_q, n_k, modes, nb, width)
    return pl.pallas_call(
        lambda *refs: rotate_kernel(*refs, n_x=n_x, n_y=n_y),
        in_specs=[
            pl.BlockSpec(memory_space=pltpu.SMEM),
            pl.BlockSpec(memory_space=pltpu.VMEM),
            pl.BlockSpec(memory_space=pltpu.HBM),
        ],
        out_specs=pl.BlockSpec(memory_space=pltpu.HBM),
        out_shape=jax.ShapeDtypeStruct(shape, jnp.bfloat16),
        scratch_shapes=stream_scratch(halves.shape, shape, R_GROUPS)
        + [pltpu.VMEM((n_k // R_GROUPS * n_q, width, width), jnp.bfloat16)] * 2
        + [pltpu.VMEM((n_k // R_GROUPS * n_q, width, pairs * width), jnp.float32)] * 2,
        compiler_params=pltpu.CompilerParams(vmem_limit_bytes=50 * MIB),
        cost_estimate=pl.CostEstimate(
            flops=4 * n_q * n_k * modes * nb * width * nb,
            bytes_accessed=4 * n_q * n_k * modes * nb * width,
            transcendentals=0,
        ),
        name="rotate",
    )(shifts, partner, halves)


def per_device(wannier, coupling, kq_map):
    rows_x, cols_y, nb, width = wannier.shape
    n_q = coupling.shape[0]
    modes = coupling.shape[3]
    count_x = lax.axis_size("kx")
    count_y = lax.axis_size("ky")
    devices = count_x * count_y
    n_k = rows_x * cols_y
    pieces = devices // n_k
    rows = nb // pieces
    total_y = cols_y * count_y
    me = lax.axis_index("kx") * count_y + lax.axis_index("ky")
    point = me // pieces
    offset = kq_map[:, 0]
    offset_x = offset // total_y
    offset_y = offset % total_y
    inner_x = offset_x % rows_x
    inner_y = offset_y % cols_y
    carry_x = (point // cols_y < inner_x).astype(jnp.int32)
    carry_y = (point % cols_y < inner_y).astype(jnp.int32)
    shifts = jnp.stack(
        [offset_x // rows_x + carry_x, offset_y // cols_y + carry_y, inner_x, inner_y], axis=1
    )

    spread = lax.all_to_all(wannier.reshape(devices, rows, width), AXES, 0, 0, tiled=True)
    halves = half_turns(
        wannier.reshape(n_k, nb, width), coupling.reshape(n_q, n_k, modes, nb, width)
    )
    outgoing = shuffle(shifts, spread.reshape(count_x, count_y, rows, width), n_q)
    back = lax.all_to_all(outgoing.reshape(devices, n_q * rows, width), AXES, 0, 0, tiled=True)
    partner = back.reshape(n_k, pieces, n_q * rows, width)
    rotated = rotate(shifts, partner, halves, rows_x, cols_y)
    return rotated.reshape(coupling.shape)


def solution(mesh):
    in_specs = (P("kx", "ky", None, None), P(None, "kx", "ky", None, None, None), P())
    out_specs = P(None, "kx", "ky", None, None, None)
    return jax.shard_map(
        per_device, mesh=mesh, in_specs=in_specs, out_specs=out_specs, check_vma=False
    )
```

```python
import jax
import jax.numpy as jnp
import numpy as np
from jax import lax
from jax.experimental import pallas as pl
from jax.experimental.pallas import tpu as pltpu
from jax.sharding import PartitionSpec as P

X_AXES = ("z_lo", "y")
Y_AXES = ("x", "z_hi", "core")
X_SIZES = (2, 4)
Y_SIZES = (4, 2, 2)
ORDER = ("core", "z_hi", "z_lo", "x", "y")
MIB = 1024 * 1024
H_GROUPS = 8
R_GROUPS = 16


def stream(in_ref, out_ref, in_buf, out_buf, in_sem, out_sem, work):
    groups = in_sem.shape[0]
    size = in_buf.shape[1] // groups

    def fetch(i):
        at = pl.ds(i * size, size)
        return pltpu.make_async_copy(in_ref.at[:, at], in_buf.at[:, at], in_sem.at[i])

    def send(i):
        at = pl.ds(i * size, size)
        return pltpu.make_async_copy(out_buf.at[:, at], out_ref.at[:, at], out_sem.at[i])

    def start(i, carry):
        fetch(i).start()
        return carry

    def step(i, carry):
        fetch(i).wait()
        for k in range(size):
            work(i * size + k)
        send(i).start()
        return carry

    def finish(i, carry):
        send(i).wait()
        return carry

    lax.fori_loop(0, groups, start, 0)
    lax.fori_loop(0, groups, step, 0)
    lax.fori_loop(0, groups, finish, 0)


def stream_scratch(shape_in, shape_out, groups):
    return [
        pltpu.VMEM(shape_in, jnp.bfloat16),
        pltpu.VMEM(shape_out, jnp.bfloat16),
        pltpu.SemaphoreType.DMA((groups,)),
        pltpu.SemaphoreType.DMA((groups,)),
    ]


def half_turn_kernel(u_ref, g_ref, o_ref, g_buf, o_buf, in_sem, out_sem):
    n_q, _, modes, nb, width = g_buf.shape

    def work(k):
        u = u_ref[k]
        turned = jnp.concatenate([-u[:, nb:], u[:, :nb]], axis=1)
        factor = jnp.concatenate([u, turned], axis=0)
        for q in range(n_q):
            rows = g_buf[q, k].reshape(modes * nb, width)
            half = jnp.dot(rows, factor, preferred_element_type=jnp.float32).astype(jnp.bfloat16)
            for p in range(modes // 2):
                one = half[2 * p * nb : (2 * p + 1) * nb]
                two = half[(2 * p + 1) * nb : (2 * p + 2) * nb]
                o_buf[q, k, :nb, p * width : (p + 1) * width] = jnp.concatenate([one[:, :nb], two[:, :nb]], axis=1)
                o_buf[q, k, nb:, p * width : (p + 1) * width] = jnp.concatenate([one[:, nb:], two[:, nb:]], axis=1)

    stream(g_ref, o_ref, g_buf, o_buf, in_sem, out_sem, work)


def half_turns(wannier, coupling):
    n_q, n_k, modes, nb, width = coupling.shape
    paired = (n_q, n_k, 2 * nb, modes // 2 * width)
    return pl.pallas_call(
        half_turn_kernel,
        in_specs=[pl.BlockSpec(memory_space=pltpu.VMEM), pl.BlockSpec(memory_space=pltpu.HBM)],
        out_specs=pl.BlockSpec(memory_space=pltpu.HBM),
        out_shape=jax.ShapeDtypeStruct(paired, jnp.bfloat16),
        scratch_shapes=stream_scratch(coupling.shape, paired, H_GROUPS),
        compiler_params=pltpu.CompilerParams(vmem_limit_bytes=56 * MIB),
        cost_estimate=pl.CostEstimate(
            flops=4 * n_q * n_k * modes * nb * width * width,
            bytes_accessed=4 * n_q * n_k * modes * nb * width,
            transcendentals=0,
        ),
        name="half_turns",
    )(wannier, coupling)


def grid_places():
    sizes = dict(zip(X_AXES + Y_AXES, X_SIZES + Y_SIZES))
    places = []
    for at in np.ndindex(*(sizes[name] for name in ORDER)):
        where = dict(zip(ORDER, at))
        x = np.ravel_multi_index([where[name] for name in X_AXES], X_SIZES)
        y = np.ravel_multi_index([where[name] for name in Y_AXES], Y_SIZES)
        places.append((int(x), int(y)))
    return places


def shuffle_kernel(shift_ref, held_ref, o_ref, twice_ref):
    n_x = twice_ref.shape[0]
    n_y = twice_ref.shape[1] // 2
    rows = held_ref.shape[1]
    number = {}
    for at, (x, y) in enumerate(grid_places()):
        number[x, y] = at
        tile = held_ref[at]
        twice_ref[x, y] = tile
        twice_ref[x, n_y + y] = tile
    for q in range(o_ref.shape[1] // rows):
        shift_x = shift_ref[q, 0]
        run = pl.ds(lax.rem(shift_ref[q, 1], n_y), n_y)
        for x in range(n_x):
            row = twice_ref[lax.rem(shift_x + x, n_x), run]
            for y in range(n_y):
                o_ref[number[x, y], q * rows : (q + 1) * rows] = row[y]


def shuffle(shifts, held, n_x, n_y, n_q):
    devices, rows, width = held.shape
    return pl.pallas_call(
        shuffle_kernel,
        in_specs=[
            pl.BlockSpec(memory_space=pltpu.SMEM),
            pl.BlockSpec(memory_space=pltpu.VMEM),
        ],
        out_specs=pl.BlockSpec(memory_space=pltpu.VMEM),
        out_shape=jax.ShapeDtypeStruct((devices, n_q * rows, width), held.dtype),
        scratch_shapes=[pltpu.VMEM((n_x, 2 * n_y, rows, width), held.dtype)],
        compiler_params=pltpu.CompilerParams(vmem_limit_bytes=8 * MIB),
        name="shuffle",
    )(shifts, held)


def rotate_kernel(
    shift_ref, v_ref, h_ref, o_ref, h_buf, o_buf, in_sem, out_sem, left_a, left_b, raw_a, raw_b, *, n_x, n_y
):
    n_q, n_k, modes, nb, width = o_buf.shape
    rows = v_ref.shape[2] // n_q
    pairs = modes // 2
    groups = in_sem.shape[0]
    size = n_k // groups
    units = [(q, k) for k in range(size) for q in range(n_q)]

    def fetch(i):
        at = pl.ds(i * size, size)
        return pltpu.make_async_copy(h_ref.at[:, at], h_buf.at[:, at], in_sem.at[i])

    def send(i):
        at = pl.ds(i * size, size)
        return pltpu.make_async_copy(o_buf.at[:, at], o_ref.at[:, at], out_sem.at[i])

    def prepare(i, left_ref):
        for u, (q, k) in enumerate(units):
            at = i * size + k
            at_x = lax.rem(at // n_y + shift_ref[q, 2], n_x)
            at_y = lax.rem(lax.rem(at, n_y) + shift_ref[q, 3], n_y)
            v = v_ref[at_x * n_y + at_y, :, q * rows : (q + 1) * rows].reshape(nb, width)
            left = jnp.concatenate(
                [
                    jnp.concatenate([v[:, :nb], -v[:, nb:]], axis=1),
                    jnp.concatenate([v[:, nb:], v[:, :nb]], axis=1),
                ],
                axis=0,
            )
            left_ref[u] = left.T

    def multiply(i, left_ref, raw_ref):
        for u, (q, k) in enumerate(units):
            right = h_buf[q, i * size + k]
            out = jnp.dot(left_ref[u], right, preferred_element_type=jnp.float32)
            raw_ref[u] = out

    lane = lax.broadcasted_iota(jnp.int32, (nb, width), 1)

    def arrange(i, raw_ref):
        for u, (q, k) in enumerate(units):
            at = i * size + k
            for p in range(pairs):
                real = raw_ref[u, :nb, p * width : (p + 1) * width]
                imag = raw_ref[u, nb:, p * width : (p + 1) * width]
                outer = jnp.where(lane < nb, real, imag)
                inner = pltpu.roll(jnp.where(lane < nb, imag, real), nb, 1)
                one = jnp.where(lane < nb, outer, inner)
                two = jnp.where(lane < nb, inner, outer)
                o_buf[q, at, 2 * p] = one.astype(jnp.bfloat16)
                o_buf[q, at, 2 * p + 1] = two.astype(jnp.bfloat16)

    def start(i, carry):
        fetch(i).start()
        return carry

    def step(j, carry):
        i = 2 * j
        last = jnp.maximum(i - 1, 0)
        fetch(i).wait()
        multiply(i, left_a, raw_a)
        prepare(i + 1, left_b)
        arrange(last, raw_b)

        @pl.when(j > 0)
        def _():
            send(last).start()

        fetch(i + 1).wait()
        multiply(i + 1, left_b, raw_b)
        prepare(jnp.minimum(i + 2, groups - 1), left_a)
        arrange(i, raw_a)
        send(i).start()
        return carry

    def finish(i, carry):
        send(i).wait()
        return carry

    lax.fori_loop(0, groups, start, 0)
    prepare(0, left_a)
    lax.fori_loop(0, groups // 2, step, 0)
    arrange(groups - 1, raw_b)
    send(groups - 1).start()
    lax.fori_loop(0, groups, finish, 0)


def rotate(shifts, partner, halves, n_x, n_y):
    n_q, n_k, width, columns = halves.shape
    pairs, nb = columns // width, width // 2
    modes = 2 * pairs
    shape = (n_q, n_k, modes, nb, width)
    return pl.pallas_call(
        lambda *refs: rotate_kernel(*refs, n_x=n_x, n_y=n_y),
        in_specs=[
            pl.BlockSpec(memory_space=pltpu.SMEM),
            pl.BlockSpec(memory_space=pltpu.VMEM),
            pl.BlockSpec(memory_space=pltpu.HBM),
        ],
        out_specs=pl.BlockSpec(memory_space=pltpu.HBM),
        out_shape=jax.ShapeDtypeStruct(shape, jnp.bfloat16),
        scratch_shapes=stream_scratch(halves.shape, shape, R_GROUPS)
        + [pltpu.VMEM((n_k // R_GROUPS * n_q, width, width), jnp.bfloat16)] * 2
        + [pltpu.VMEM((n_k // R_GROUPS * n_q, width, pairs * width), jnp.float32)] * 2,
        compiler_params=pltpu.CompilerParams(vmem_limit_bytes=50 * MIB),
        cost_estimate=pl.CostEstimate(
            flops=4 * n_q * n_k * modes * nb * width * nb,
            bytes_accessed=4 * n_q * n_k * modes * nb * width,
            transcendentals=0,
        ),
        name="rotate",
    )(shifts, partner, halves)


def per_device(wannier, coupling, kq_map):
    rows_x, cols_y, nb, width = wannier.shape
    n_q = coupling.shape[0]
    modes = coupling.shape[3]
    count_x = lax.axis_size(X_AXES)
    count_y = lax.axis_size(Y_AXES)
    devices = count_x * count_y
    n_k = rows_x * cols_y
    pieces = devices // n_k
    rows = nb // pieces
    total_y = cols_y * count_y
    me = lax.axis_index(ORDER)
    point = me // pieces
    offset = kq_map[:, 0]
    offset_x = offset // total_y
    offset_y = offset % total_y
    inner_x = offset_x % rows_x
    inner_y = offset_y % cols_y
    carry_x = (point // cols_y < inner_x).astype(jnp.int32)
    carry_y = (point % cols_y < inner_y).astype(jnp.int32)
    shifts = jnp.stack(
        [offset_x // rows_x + carry_x, offset_y // cols_y + carry_y, inner_x, inner_y], axis=1
    )

    spread = lax.all_to_all(wannier.reshape(devices, rows, width), ORDER, 0, 0, tiled=True)
    halves = half_turns(
        wannier.reshape(n_k, nb, width), coupling.reshape(n_q, n_k, modes, nb, width)
    )
    outgoing = shuffle(shifts, spread, count_x, count_y, n_q)
    back = lax.all_to_all(outgoing, ORDER, 0, 0, tiled=True)
    partner = back.reshape(n_k, pieces, n_q * rows, width)
    rotated = rotate(shifts, partner, halves, rows_x, cols_y)
    return rotated.reshape(coupling.shape)


def solution(mesh):
    links = jax.sharding.Mesh(
        mesh.devices.reshape(X_SIZES + Y_SIZES), X_AXES + Y_AXES, axis_types=mesh.axis_types[:1] * 5
    )
    in_specs = (P(X_AXES, Y_AXES), P(None, X_AXES, Y_AXES), P())
    out_specs = P(None, X_AXES, Y_AXES)
    return jax.shard_map(
        per_device, mesh=links, in_specs=in_specs, out_specs=out_specs, check_vma=False
    )
```

```python
import jax
import jax.numpy as jnp
import numpy as np
from jax import lax
from jax.experimental import pallas as pl
from jax.experimental.pallas import tpu as pltpu
from jax.sharding import PartitionSpec as P

X_AXES = ("z_lo", "y")
Y_AXES = ("x", "z_hi", "core")
X_SIZES = (2, 4)
Y_SIZES = (4, 2, 2)
ORDER = ("core", "z_hi", "z_lo", "x", "y")
MIB = 1024 * 1024
H_GROUPS = 8
R_GROUPS = 16


def stream(in_ref, out_ref, in_buf, out_buf, in_sem, out_sem, work):
    groups = in_sem.shape[0]
    size = in_buf.shape[1] // groups

    def fetch(i):
        at = pl.ds(i * size, size)
        return pltpu.make_async_copy(in_ref.at[:, at], in_buf.at[:, at], in_sem.at[i])

    def send(i):
        at = pl.ds(i * size, size)
        return pltpu.make_async_copy(out_buf.at[:, at], out_ref.at[:, at], out_sem.at[i])

    def start(i, carry):
        fetch(i).start()
        return carry

    def step(i, carry):
        fetch(i).wait()
        for k in range(size):
            work(i * size + k)
        send(i).start()
        return carry

    def finish(i, carry):
        send(i).wait()
        return carry

    lax.fori_loop(0, groups, start, 0)
    lax.fori_loop(0, groups, step, 0)
    lax.fori_loop(0, groups, finish, 0)


def stream_scratch(shape_in, shape_out, groups):
    return [
        pltpu.VMEM(shape_in, jnp.bfloat16),
        pltpu.VMEM(shape_out, jnp.bfloat16),
        pltpu.SemaphoreType.DMA(groups),
        pltpu.SemaphoreType.DMA(groups),
    ]


def half_turn_kernel(u_ref, g_ref, o_ref, g_buf, o_buf, in_sem, out_sem):
    n_q, _, modes, nb, width = g_buf.shape

    def work(k):
        u = u_ref[k]
        turned = jnp.concatenate([-u[:, nb:], u[:, :nb]], axis=1)
        factor = jnp.concatenate([u, turned], axis=0)
        for q in range(n_q):
            rows = g_buf[q, k].reshape(modes * nb, width)
            half = jnp.dot(rows, factor, preferred_element_type=jnp.float32).astype(jnp.bfloat16)
            for p in range(modes // 2):
                one = half[2 * p * nb : (2 * p + 1) * nb]
                two = half[(2 * p + 1) * nb : (2 * p + 2) * nb]
                o_buf[q, k, :nb, p * width : (p + 1) * width] = jnp.concatenate([one[:, :nb], two[:, :nb]], axis=1)
                o_buf[q, k, nb:, p * width : (p + 1) * width] = jnp.concatenate([one[:, nb:], two[:, nb:]], axis=1)

    stream(g_ref, o_ref, g_buf, o_buf, in_sem, out_sem, work)


def half_turns(wannier, coupling):
    n_q, n_k, modes, nb, width = coupling.shape
    paired = (n_q, n_k, 2 * nb, modes // 2 * width)
    return pl.pallas_call(
        half_turn_kernel,
        in_specs=[pl.BlockSpec(memory_space=pltpu.VMEM), pl.BlockSpec(memory_space=pltpu.HBM)],
        out_specs=pl.BlockSpec(memory_space=pltpu.HBM),
        out_shape=jax.ShapeDtypeStruct(paired, jnp.bfloat16),
        scratch_shapes=stream_scratch(coupling.shape, paired, (H_GROUPS,)),
        compiler_params=pltpu.CompilerParams(vmem_limit_bytes=56 * MIB),
        cost_estimate=pl.CostEstimate(
            flops=4 * n_q * n_k * modes * nb * width * width,
            bytes_accessed=4 * n_q * n_k * modes * nb * width,
            transcendentals=0,
        ),
        name="half_turns",
    )(wannier, coupling)


def grid_places():
    sizes = dict(zip(X_AXES + Y_AXES, X_SIZES + Y_SIZES))
    places = []
    for at in np.ndindex(*(sizes[name] for name in ORDER)):
        where = dict(zip(ORDER, at))
        x = np.ravel_multi_index([where[name] for name in X_AXES], X_SIZES)
        y = np.ravel_multi_index([where[name] for name in Y_AXES], Y_SIZES)
        places.append((int(x), int(y)))
    return places


def shuffle_kernel(shift_ref, held_ref, o_ref, twice_ref):
    n_x = twice_ref.shape[0]
    n_y = twice_ref.shape[1] // 2
    rows = held_ref.shape[1]
    number = {}
    for at, (x, y) in enumerate(grid_places()):
        number[x, y] = at
        tile = held_ref[at]
        twice_ref[x, y] = tile
        twice_ref[x, n_y + y] = tile
    for q in range(o_ref.shape[1] // rows):
        shift_x = shift_ref[q, 0]
        run = pl.ds(lax.rem(shift_ref[q, 1], n_y), n_y)
        for x in range(n_x):
            row = twice_ref[lax.rem(shift_x + x, n_x), run]
            for y in range(n_y):
                o_ref[number[x, y], q * rows : (q + 1) * rows] = row[y]


def shuffle(shifts, held, n_x, n_y, n_q):
    devices, rows, width = held.shape
    return pl.pallas_call(
        shuffle_kernel,
        in_specs=[
            pl.BlockSpec(memory_space=pltpu.SMEM),
            pl.BlockSpec(memory_space=pltpu.VMEM),
        ],
        out_specs=pl.BlockSpec(memory_space=pltpu.VMEM),
        out_shape=jax.ShapeDtypeStruct((devices, n_q * rows, width), held.dtype),
        scratch_shapes=[pltpu.VMEM((n_x, 2 * n_y, rows, width), held.dtype)],
        compiler_params=pltpu.CompilerParams(vmem_limit_bytes=8 * MIB),
        name="shuffle",
    )(shifts, held)


def rotate_kernel(
    shift_ref, v_ref, h_ref, o_ref, h_buf, o_buf, in_sem, out_sem, left_a, left_b, raw_a, raw_b, *, n_x, n_y
):
    n_q, n_k, modes, nb, width = o_buf.shape
    rows = v_ref.shape[2] // n_q
    pairs = modes // 2
    groups = in_sem.shape[0]
    size = n_k // groups
    units = [(q, k) for k in range(size) for q in range(n_q)]

    def fetch(i, q):
        at = pl.ds(i * size, size)
        return pltpu.make_async_copy(h_ref.at[q, at], h_buf.at[q, at], in_sem.at[i, q])

    def send(i, q):
        at = pl.ds(i * size, size)
        return pltpu.make_async_copy(o_buf.at[q, at], o_ref.at[q, at], out_sem.at[i, q])

    def each(copy, i, action):
        for q in range(n_q):
            getattr(copy(i, q), action)()

    def prepare(i, left_ref):
        for u, (q, k) in enumerate(units):
            at = i * size + k
            at_x = lax.rem(at // n_y + shift_ref[q, 2], n_x)
            at_y = lax.rem(lax.rem(at, n_y) + shift_ref[q, 3], n_y)
            v = v_ref[at_x * n_y + at_y, :, q * rows : (q + 1) * rows].reshape(nb, width)
            left = jnp.concatenate(
                [
                    jnp.concatenate([v[:, :nb], -v[:, nb:]], axis=1),
                    jnp.concatenate([v[:, nb:], v[:, :nb]], axis=1),
                ],
                axis=0,
            )
            left_ref[u] = left.T

    def multiply(i, left_ref, raw_ref):
        for u, (q, k) in enumerate(units):
            right = h_buf[q, i * size + k]
            out = jnp.dot(left_ref[u], right, preferred_element_type=jnp.float32)
            raw_ref[u] = out

    lane = lax.broadcasted_iota(jnp.int32, (nb, width), 1)

    def arrange(i, raw_ref):
        for u, (q, k) in enumerate(units):
            at = i * size + k
            for p in range(pairs):
                real = raw_ref[u, :nb, p * width : (p + 1) * width]
                imag = raw_ref[u, nb:, p * width : (p + 1) * width]
                outer = jnp.where(lane < nb, real, imag)
                inner = pltpu.roll(jnp.where(lane < nb, imag, real), nb, 1)
                one = jnp.where(lane < nb, outer, inner)
                two = jnp.where(lane < nb, inner, outer)
                o_buf[q, at, 2 * p] = one.astype(jnp.bfloat16)
                o_buf[q, at, 2 * p + 1] = two.astype(jnp.bfloat16)

    def start(i, carry):
        each(fetch, i, "start")
        return carry

    def step(j, carry):
        i = 2 * j
        last = jnp.maximum(i - 1, 0)
        each(fetch, i, "wait")
        multiply(i, left_a, raw_a)
        prepare(i + 1, left_b)
        arrange(last, raw_b)

        @pl.when(j > 0)
        def _():
            each(send, last, "start")

        each(fetch, i + 1, "wait")
        multiply(i + 1, left_b, raw_b)
        prepare(jnp.minimum(i + 2, groups - 1), left_a)
        arrange(i, raw_a)
        each(send, i, "start")
        return carry

    def finish(i, carry):
        each(send, i, "wait")
        return carry

    lax.fori_loop(0, groups, start, 0)
    prepare(0, left_a)
    lax.fori_loop(0, groups // 2, step, 0)
    arrange(groups - 1, raw_b)
    each(send, groups - 1, "start")
    lax.fori_loop(0, groups, finish, 0)


def rotate(shifts, partner, halves, n_x, n_y):
    n_q, n_k, width, columns = halves.shape
    pairs, nb = columns // width, width // 2
    modes = 2 * pairs
    shape = (n_q, n_k, modes, nb, width)
    return pl.pallas_call(
        lambda *refs: rotate_kernel(*refs, n_x=n_x, n_y=n_y),
        in_specs=[
            pl.BlockSpec(memory_space=pltpu.SMEM),
            pl.BlockSpec(memory_space=pltpu.VMEM),
            pl.BlockSpec(memory_space=pltpu.HBM),
        ],
        out_specs=pl.BlockSpec(memory_space=pltpu.HBM),
        out_shape=jax.ShapeDtypeStruct(shape, jnp.bfloat16),
        scratch_shapes=stream_scratch(halves.shape, shape, (R_GROUPS, n_q))
        + [pltpu.VMEM((n_k // R_GROUPS * n_q, width, width), jnp.bfloat16)] * 2
        + [pltpu.VMEM((n_k // R_GROUPS * n_q, width, pairs * width), jnp.float32)] * 2,
        compiler_params=pltpu.CompilerParams(vmem_limit_bytes=50 * MIB),
        cost_estimate=pl.CostEstimate(
            flops=4 * n_q * n_k * modes * nb * width * nb,
            bytes_accessed=4 * n_q * n_k * modes * nb * width,
            transcendentals=0,
        ),
        name="rotate",
    )(shifts, partner, halves)


def per_device(wannier, coupling, kq_map):
    rows_x, cols_y, nb, width = wannier.shape
    n_q = coupling.shape[0]
    modes = coupling.shape[3]
    count_x = lax.axis_size(X_AXES)
    count_y = lax.axis_size(Y_AXES)
    devices = count_x * count_y
    n_k = rows_x * cols_y
    pieces = devices // n_k
    rows = nb // pieces
    total_y = cols_y * count_y
    me = lax.axis_index(ORDER)
    point = me // pieces
    offset = kq_map[:, 0]
    offset_x = offset // total_y
    offset_y = offset % total_y
    inner_x = offset_x % rows_x
    inner_y = offset_y % cols_y
    carry_x = (point // cols_y < inner_x).astype(jnp.int32)
    carry_y = (point % cols_y < inner_y).astype(jnp.int32)
    shifts = jnp.stack(
        [offset_x // rows_x + carry_x, offset_y // cols_y + carry_y, inner_x, inner_y], axis=1
    )

    spread = lax.all_to_all(wannier.reshape(devices, rows, width), ORDER, 0, 0, tiled=True)
    halves = half_turns(
        wannier.reshape(n_k, nb, width), coupling.reshape(n_q, n_k, modes, nb, width)
    )
    outgoing = shuffle(shifts, spread, count_x, count_y, n_q)
    back = lax.all_to_all(outgoing, ORDER, 0, 0, tiled=True)
    partner = back.reshape(n_k, pieces, n_q * rows, width)
    rotated = rotate(shifts, partner, halves, rows_x, cols_y)
    return rotated.reshape(coupling.shape)


def solution(mesh):
    links = jax.sharding.Mesh(
        mesh.devices.reshape(X_SIZES + Y_SIZES), X_AXES + Y_AXES, axis_types=mesh.axis_types[:1] * 5
    )
    in_specs = (P(X_AXES, Y_AXES), P(None, X_AXES, Y_AXES), P())
    out_specs = P(None, X_AXES, Y_AXES)
    return jax.shard_map(
        per_device, mesh=links, in_specs=in_specs, out_specs=out_specs, check_vma=False
    )
```
